128 devices in a mesh: member: 8 (over y, core), shard: 16 (over z, x).
Axes of the slice: x: 4, y: 4, z: 4, core: 2. Of those that a mesh axis runs over, the one named last changes fastest.
Arguments:
- member_grams: float32 [8, 4096, 4096], P('member', 'shard'), as said below
- member_weights: bfloat16 [8, 4096, 2304], P('member', 'shard'), may hold values from -6 to 6
Outputs:
- merged: float32 [4096, 2304], P('shard', 'member')
The draws below stay inside these ranges and needn't reach their ends.
Inputs may be any that keep to these rules, and one draw needn't show every extreme that they name: `member_grams`: each member's matrix is symmetric positive definite.
All inputs are finite; a program needn't handle non-finite values.
Results may differ from the reference program's by a relative error of at most 0.0032.
Values may be sent and summed in bfloat16 or wider, within the bound.
No kernel may reach another device: no remote copies, remote signals or barrier semaphores. Data moves between devices by JAX's collectives and lax.ppermute only.
A program may use at most 128 MiB of HBM per device.

```python
import math
import jax
import jax.numpy as jnp
from jax import lax

K = 4096
OUT = 2304
ITERS = 3
MEMBERS = 8


def draw_member_grams(key, part):
    samples = K // 4
    key_rows = jax.random.fold_in(key, 11)
    key_scales = jax.random.fold_in(key, 23)
    key_coupled = jax.random.fold_in(key, 37)
    key_strength = jax.random.fold_in(key, 41)
    position = jnp.arange(K, dtype=jnp.float32) / K
    strength = jnp.exp(jax.random.uniform(key_strength, (MEMBERS, 1, 2), jnp.float32, math.log(10.0), math.log(80.0)))
    factors = jax.random.normal(key_rows, (MEMBERS, K, samples), jnp.float32)
    spread = jax.random.uniform(key_scales, (MEMBERS, K), jnp.float32, 0.0, math.log(3.3))
    scales = jnp.exp(spread) * jnp.exp(position * math.log(3.0))[None, :]
    coupled = jax.random.normal(key_coupled, (MEMBERS, K, 2), jnp.float32)
    coupled = coupled * jnp.sqrt(strength)
    covariance = jnp.einsum('mks,mjs->mkj', factors, factors, precision=lax.Precision.HIGHEST) / samples
    covariance = covariance + jnp.einsum('mks,mjs->mkj', coupled, coupled, precision=lax.Precision.HIGHEST) / K
    covariance = covariance + 2.0 * jnp.eye(K, dtype=jnp.float32)[None, :, :]
    scaled = covariance * scales[:, :, None] * scales[:, None, :]
    return 0.5 * (scaled + jnp.swapaxes(scaled, 1, 2))


def block_scale(rng, dims, split, low, high):
    factor_of = 1.0
    for dim, shards_of in split:
        steps = jax.random.uniform(jax.random.fold_in(jax.random.fold_in(rng, 6), dim), (shards_of,), jnp.float32, low / len(split), high / len(split))
        factor_of = factor_of * jnp.repeat(jnp.exp(steps), dims[dim] // shards_of).reshape((-1,) + (1,) * (len(dims) - 1 - dim))
    return factor_of


def normal_values(stream_key, extent, scale, limit, pieces=(), held_as=jnp.bfloat16):
    result = jax.random.normal(stream_key, extent, jnp.float32) * scale
    if len(pieces) > 0:
        result = block_scale(stream_key, extent, pieces, -0.22, 0.18) * result
    return jnp.clip(result, min=-limit, max=limit).astype(held_as)


def setup_inputs(seed: int = 0) -> dict:
    key_of = jax.random.split(jax.random.key(seed), 3)
    member_grams = draw_member_grams(jax.random.fold_in(key_of[2], 71), 0)
    member_weights = normal_values(key_of[1], (MEMBERS, K, OUT), 1.0, 6.0, ((0, 8), (1, 16)))
    return dict(member_grams=member_grams, member_weights=member_weights)


shrink = 0.9


def regularize(gram_block, row_offset):
    height = gram_block.shape[-2]
    width = gram_block.shape[-1]
    row_index = lax.broadcasted_iota(jnp.int32, (height, width), 0) + row_offset
    col_index = lax.broadcasted_iota(jnp.int32, (height, width), 1)
    return jnp.where(row_index == col_index, gram_block, shrink * gram_block)


def reference(member_grams, member_weights):
    def accumulate(carry, member):
        gram_matrix, weight_matrix = member
        regular = regularize(gram_matrix, 0)
        gram_low = lax.optimization_barrier(regular.astype(jnp.bfloat16))
        rhs_term = jnp.dot(gram_low.astype(jnp.float32), weight_matrix.astype(jnp.float32),
                           precision=lax.Precision.HIGHEST, preferred_element_type=jnp.float32)
        return (carry[0] + regular, carry[1] + rhs_term), None

    start_carry = (jnp.zeros((K, K), jnp.float32), jnp.zeros((K, OUT), jnp.float32))
    (gram_sum, right_side), unused = lax.scan(accumulate, start_carry, (member_grams, member_weights))
    merged = jnp.zeros((K, OUT), jnp.float32)
    residual = right_side
    direction = right_side
    norm_now = jnp.sum(residual * residual, axis=0)
    for iteration in range(ITERS):
        images = jnp.dot(gram_sum, direction, precision=lax.Precision.HIGHEST,
                         preferred_element_type=jnp.float32)
        step_size = norm_now / jnp.sum(direction * images, axis=0)
        merged = merged + step_size * direction
        residual = residual - step_size * images
        if iteration + 1 < ITERS:
            norm_next = jnp.sum(residual * residual, axis=0)
            direction = residual + (norm_next / norm_now) * direction
            norm_now = norm_next
    return merged
```

```python
import functools
import jax
import jax.numpy as jnp
from jax import lax
from jax.experimental import pallas as pl
from jax.experimental.pallas import tpu as pltpu
from jax.sharding import Mesh, PartitionSpec as P

MEMBER = ("y", "core")
SHARD = ("z", "x")
ALL = ("y", "core", "z", "x")
SIZES = (4, 2, 4, 4)
SHRINK = 0.9
ROWS = 256
CHUNK = 512
COLS = 144
SPARE = 8
F32 = jnp.float32
BF16 = jnp.bfloat16


def exchange(parts, axis):
    return lax.all_to_all(parts, axis, split_axis=0, concat_axis=0, tiled=True)


def turn(block, axis, step):
    size = lax.axis_size(axis)
    return lax.ppermute(block, axis, [(i, (i + step) % size) for i in range(size)])


def dot(a, b):
    return jnp.dot(a, b, preferred_element_type=F32)


def spread_grams(gram, place):
    row = lax.broadcasted_iota(jnp.int32, gram.shape, 0) + place * ROWS
    col = lax.broadcasted_iota(jnp.int32, gram.shape, 1)
    on = row == col
    regular = jnp.where(on, gram, SHRINK * gram)
    low = regular.astype(BF16)
    rest = jnp.sum(jnp.where(on, regular - low.astype(F32), 0.0), axis=0, keepdims=True)
    rest = jnp.pad(rest, ((0, SPARE - 1), (0, 0))).astype(BF16)
    blocks = jnp.concatenate([low, rest], axis=0)
    return blocks.reshape(ROWS + SPARE, -1, CHUNK).transpose(1, 0, 2)


def sum_grams(blocks, place, chunk):
    total = jnp.sum(blocks.astype(F32), axis=0)
    block, rest = total[:ROWS], total[ROWS : ROWS + 1]
    row = lax.broadcasted_iota(jnp.int32, block.shape, 0) + place * ROWS
    col = lax.broadcasted_iota(jnp.int32, block.shape, 1) + chunk * CHUNK
    low = block.astype(BF16)
    rest = rest + jnp.sum(jnp.where(row == col, block - low.astype(F32), 0.0), axis=0, keepdims=True)
    rest = jnp.pad(rest, ((0, SPARE - 1), (0, 0))).astype(BF16)
    return jnp.concatenate([low, rest], axis=0)


def right_side_kernel(w_ref, g_ref, out_ref):
    total = dot(w_ref[0], g_ref[0, :ROWS])
    for m in range(1, w_ref.shape[0]):
        total += dot(w_ref[m], g_ref[m, :ROWS])
    out_ref[...] = total.astype(BF16).reshape(out_ref.shape)


def right_side_parts(weights, grams):
    members, outs, _ = weights.shape
    step = 4
    return pl.pallas_call(
        right_side_kernel,
        grid=(outs // (step * COLS),),
        in_specs=[
            pl.BlockSpec((members, step * COLS, ROWS), lambda i: (0, i, 0)),
            pl.BlockSpec(grams.shape, lambda i: (0, 0, 0)),
        ],
        out_specs=pl.BlockSpec((step, COLS, CHUNK), lambda i: (i, 0, 0)),
        out_shape=jax.ShapeDtypeStruct((outs // COLS, COLS, CHUNK), BF16),
        name="right_side",
    )(weights, grams)


def product_kernel(pos_ref, gram_ref, diag_ref, own_ref, *refs):
    blocks, out_ref = refs[:-1], refs[-1]
    y, core = pos_ref[0], pos_ref[1]
    own = own_ref[...]
    total = jnp.zeros(own.shape, F32)
    for i, ref in enumerate(blocks):
        at = lax.rem(y + 4 - i % 4, 4) * 2 + (core if i < 4 else 1 - core)
        for half in range(2):
            total += dot(ref[:, half * ROWS : (half + 1) * ROWS], gram_ref[2 * at + half, :ROWS])
    out_ref[...] = total + diag_ref[0:1] * (own - blocks[0][...].astype(F32)) + diag_ref[1:2] * own


def apply_gram(pos, grams, diag, own, blocks):
    return pl.pallas_call(
        product_kernel,
        in_specs=[pl.BlockSpec(memory_space=pltpu.SMEM)] + [pl.BlockSpec(memory_space=pltpu.VMEM)] * (3 + len(blocks)),
        out_specs=pl.BlockSpec(memory_space=pltpu.VMEM),
        out_shape=jax.ShapeDtypeStruct(own.shape, F32),
        name="apply_gram",
    )(pos, grams, diag, own, *blocks)


def gather(block):
    mine = [block] + [turn(block, "y", step) for step in (1, 2, 3)]
    return mine + [turn(b, "core", 1) for b in mine]


def to_output(block):
    index = lambda y, core, z, x: ((y * 2 + core) * 4 + z) * 4 + x
    places = [(y, c, z, x) for y in range(4) for c in range(2) for z in range(4) for x in range(4)]
    odd = lax.axis_index("x") % 2
    halves = [block[:, :ROWS], block[:, ROWS:]]
    came = []
    for a in range(2):
        pairs = [
            (index(y, c, z, x), index(z, x // 2, y, 2 * c + ((x % 2) ^ a))) for y, c, z, x in places
        ]
        sent = jnp.where(odd == a, halves[0], halves[1])
        came.append(lax.ppermute(sent, ALL, pairs))
    first = jnp.where(odd == 0, came[0], came[1])
    second = jnp.where(odd == 0, came[1], came[0])
    return jnp.concatenate([first, second], axis=0).T


def column_sums(a, b):
    return jnp.sum(a * b, axis=1, keepdims=True)


def whole_sums(left, right):
    return sum(column_sums(a, b) for a, b in zip(left, right))


def shards(member_grams, member_weights):
    y, core = lax.axis_index("y"), lax.axis_index("core")
    chunk = lax.axis_index(MEMBER)
    place = lax.axis_index(SHARD)
    pos = jnp.stack([y, core]).astype(jnp.int32)

    weights = lax.all_gather(member_weights[0].T, MEMBER, axis=0)
    grams = exchange(spread_grams(member_grams[0], place), MEMBER)
    gram_sum = lax.all_gather(sum_grams(grams, place, chunk), SHARD, axis=0)
    parts = exchange(right_side_parts(weights, grams), SHARD)
    r0 = jnp.sum(parts.astype(F32), axis=0)

    near = lax.dynamic_slice(gram_sum, (2 * chunk, 0, 0), (2, ROWS + SPARE, CHUNK)).astype(F32)
    row = lax.broadcasted_iota(jnp.int32, (ROWS, ROWS), 0)
    col = lax.broadcasted_iota(jnp.int32, (ROWS, ROWS), 1)
    diag = jnp.concatenate(
        [
            jnp.sum(jnp.where(row == col, near[h, :ROWS, h * ROWS : (h + 1) * ROWS], 0.0), axis=0)
            for h in range(2)
        ]
    )
    diag = jnp.stack([diag, near[0, ROWS] + near[1, ROWS]])
    diag = jnp.pad(diag, ((0, 6), (0, 0)))

    def product(own):
        blocks = gather(own.astype(BF16))
        return apply_gram(pos, gram_sum, diag, own, blocks), [b.astype(F32) for b in blocks]

    w0, r0_all = product(r0)
    z0, w0_all = product(w0)
    norm0 = whole_sums(r0_all, r0_all)
    step0 = norm0 / whole_sums(r0_all, w0_all)
    r1 = r0 - step0 * w0
    w1 = w0 - step0 * z0
    q1, w1_all = product(w1)
    r1_all = [r - step0 * w for r, w in zip(r0_all, w0_all)]
    norm1 = whole_sums(r1_all, r1_all)
    beta1 = norm1 / norm0
    step1 = norm1 / (whole_sums(r1_all, w1_all) - beta1 * norm1 / step0)
    s1 = w1 + beta1 * w0
    z1 = q1 + beta1 * z0
    p1 = r1 + beta1 * r0
    r2 = r1 - step1 * s1
    w2 = w1 - step1 * z1
    both = jnp.concatenate([column_sums(r2, r2), column_sums(r2, w2)], axis=1).T
    both = jnp.sum(exchange(jnp.broadcast_to(both, (8, 1, 2, COLS)), MEMBER), axis=(0, 1))
    norm2, curve2 = both[0][:, None], both[1][:, None]
    beta2 = norm2 / norm1
    step2 = norm2 / (curve2 - beta2 * norm2 / step1)
    p2 = r2 + beta2 * p1
    return to_output(step0 * r0 + step1 * p1 + step2 * p2)


def solution(mesh):
    fine = Mesh(mesh.devices.reshape(SIZES), ALL)
    return jax.shard_map(
        shards,
        mesh=fine,
        in_specs=(P(MEMBER, SHARD, None), P(MEMBER, SHARD, None)),
        out_specs=P(SHARD, MEMBER),
        check_vma=False,
    )
```

```python
import jax
import jax.numpy as jnp
from jax import lax
from jax.experimental import pallas as pl
from jax.experimental.pallas import tpu as pltpu
from jax.sharding import Mesh, PartitionSpec as P

MEMBER = ("y", "core")
SHARD = ("z", "x")
ALL = ("y", "core", "z", "x")
SIZES = (4, 2, 4, 4)
SHRINK = 0.9
ROWS = 256
CHUNK = 512
COLS = 144
PIECES = (80, 64)
SPARE = 16
FULL = ROWS + SPARE
F32 = jnp.float32
BF16 = jnp.bfloat16
VMEM = pl.BlockSpec(memory_space=pltpu.VMEM)
SMEM = pl.BlockSpec(memory_space=pltpu.SMEM)


def exchange(parts, axis):
    return lax.all_to_all(parts, axis, split_axis=0, concat_axis=0, tiled=True)


def turn(block, axis, step):
    size = lax.axis_size(axis)
    return lax.ppermute(block, axis, [(i, (i + step) % size) for i in range(size)])


def dot(a, b):
    return jnp.dot(a, b, preferred_element_type=F32)


def cost(flops, moved):
    return pl.CostEstimate(flops=flops, bytes_accessed=moved, transcendentals=0)


def spare_rows(first, second):
    index = lax.broadcasted_iota(jnp.int32, (SPARE, first.shape[-1]), 0)
    return jnp.where(index == 0, first, jnp.where(index == 1, second, 0.0)).astype(BF16)


def transposed(weights):
    blocks = weights.shape[1] // COLS
    group = 8
    def body(w_ref, *out_refs):
        turned = w_ref[...].astype(F32).T.astype(BF16)
        for b in range(group):
            at = b * COLS
            for out_ref, piece in zip(out_refs, PIECES):
                out_ref[b * piece : (b + 1) * piece] = turned[at : at + piece]
                at += piece
    return pl.pallas_call(
        body,
        grid=(blocks // group,),
        in_specs=[pl.BlockSpec((ROWS, group * COLS), lambda i: (0, i))],
        out_specs=[pl.BlockSpec((group * p, ROWS), lambda i: (i, 0)) for p in PIECES],
        out_shape=[jax.ShapeDtypeStruct((blocks * p, ROWS), BF16) for p in PIECES],
        cost_estimate=cost(10**8, 2 * weights.size * 2),
        name="turn_weights",
    )(weights)


def spread_kernel(pos_ref, gram_ref, out_ref):
    gram = gram_ref[...]
    row = lax.broadcasted_iota(jnp.int32, gram.shape, 0) + pos_ref[3] * ROWS
    col = lax.broadcasted_iota(jnp.int32, gram.shape, 1) + pl.program_id(0) * CHUNK
    on = row == col
    regular = jnp.where(on, gram, SHRINK * gram)
    low = regular.astype(BF16)
    rest = jnp.sum(jnp.where(on, regular - low.astype(F32), 0.0), axis=0, keepdims=True)
    out_ref[0, :ROWS] = low
    out_ref[0, ROWS:] = spare_rows(rest, jnp.zeros_like(rest))


def spread_grams(pos, gram):
    chunks = gram.shape[1] // CHUNK
    return pl.pallas_call(
        spread_kernel,
        grid=(chunks,),
        in_specs=[SMEM, pl.BlockSpec((ROWS, CHUNK), lambda i: (0, i))],
        out_specs=pl.BlockSpec((1, FULL, CHUNK), lambda i: (i, 0, 0)),
        out_shape=jax.ShapeDtypeStruct((chunks, FULL, CHUNK), BF16),
        cost_estimate=cost(10**8, gram.size * 6),
        name="spread_grams",
    )(pos, gram)


def sum_kernel(pos_ref, blocks_ref, *out_refs):
    total = jnp.sum(blocks_ref[...].astype(F32), axis=0)
    block, rest = total[:ROWS], total[ROWS : ROWS + 1]
    row = lax.broadcasted_iota(jnp.int32, block.shape, 0) + pos_ref[3] * ROWS
    col = lax.broadcasted_iota(jnp.int32, block.shape, 1) + pos_ref[4] * CHUNK
    on = row == col
    low = block.astype(BF16)
    kept = low.astype(F32)
    diag = jnp.sum(jnp.where(on, kept, 0.0), axis=0, keepdims=True)
    rest = rest + jnp.sum(jnp.where(on, block - kept, 0.0), axis=0, keepdims=True)
    spare = spare_rows(diag, rest)
    half = CHUNK // 2
    for h, out_ref in enumerate(out_refs):
        out_ref[:ROWS] = low[:, h * half : (h + 1) * half]
        out_ref[ROWS:] = spare[:, h * half : (h + 1) * half]


def sum_grams(pos, blocks):
    half = jax.ShapeDtypeStruct((FULL, CHUNK // 2), BF16)
    return pl.pallas_call(
        sum_kernel,
        in_specs=[SMEM, VMEM],
        out_specs=[VMEM, VMEM],
        out_shape=[half, half],
        cost_estimate=cost(10**8, blocks.size * 2),
        name="sum_grams",
    )(pos, blocks)


def gather_grams(halves):
    out = []
    for half, (first, second) in zip(halves, (("x", "z"), ("z", "x"))):
        line = jnp.stack([half] + [turn(half, first, step) for step in (1, 2, 3)])
        out += [line] + [turn(line, second, step) for step in (1, 2, 3)]
    return out


def gather_weights(piece):
    middle = piece.shape[0] // 2
    up, down = turn(piece, "y", 1), turn(piece, "y", 3)
    far = [turn(up[:middle], "y", 1), turn(down[middle:], "y", 3)]
    mine = [piece, up, down] + far
    return mine + [turn(b, "core", 1) for b in mine]


def right_side_kernel(pos_ref, g_ref, *refs):
    blocks, out_ref = refs[:-1], refs[-1]
    y, core = pos_ref[0], pos_ref[1]
    grams = []
    for other in range(2):
        for step in (0, 3, 1, 2):
            grams.append(g_ref.at[2 * lax.rem(y + step, 4) + (1 - core if other else core)])
    middle = out_ref.shape[0] // 2
    for part in range(2):
        rows = slice(part * middle, (part + 1) * middle)
        total = jnp.zeros((middle, out_ref.shape[1]), F32)
        for other in range(2):
            five = blocks[5 * other : 5 * other + 5]
            for k in range(3):
                total += dot(five[k][rows], grams[4 * other + k][:ROWS])
            total += dot(five[3 + part][...], grams[4 * other + 3][:ROWS])
        out_ref[rows] = total.astype(BF16)


def right_side_part(pos, grams, blocks):
    rows = blocks[0].shape[0]
    return pl.pallas_call(
        right_side_kernel,
        in_specs=[SMEM, VMEM] + [VMEM] * len(blocks),
        out_specs=VMEM,
        out_shape=jax.ShapeDtypeStruct((rows, CHUNK), BF16),
        cost_estimate=cost(2 * rows * CHUNK * ROWS * 8, rows * ROWS * 16 + grams.size * 2 + rows * CHUNK * 2),
        name="right_side",
    )(pos, grams, *blocks)


def gather(block):
    mine = [block] + [turn(block, "y", step) for step in (1, 2, 3)]
    return mine + [turn(b, "core", 1) for b in mine]


def wide(column):
    return jnp.broadcast_to(column, (column.shape[0], 128))


def product(pos_ref, gram_refs, blocks, own, all_ref):
    y, core, z, x = (pos_ref[i] for i in (0, 1, 5, 6))
    for i, ref in enumerate(blocks):
        at = lax.rem(y + 4 - i % 4, 4) * 2 + (core if i < 4 else 1 - core)
        all_ref[2 * at] = ref[:, :ROWS]
        all_ref[2 * at + 1] = ref[:, ROWS:]
    sums = []
    spare = []
    for half in range(2):
        total = jnp.zeros((own.shape[0], CHUNK // 2), F32)
        extra = jnp.zeros((8, CHUNK // 2), F32)
        for a in range(4):
            for b in range(4):
                k, j = (a, b) if half == 0 else (b, a)
                at = 4 * lax.rem(z + 4 - k, 4) + lax.rem(x + 4 - j, 4)
                ref = gram_refs[4 * half + a]
                total += dot(all_ref[at], ref[b, :ROWS])
                extra += ref[b, ROWS:].astype(F32)[:8]
        sums.append(total)
        spare.append(extra)
    total = jnp.concatenate(sums, axis=1)
    diag = jnp.concatenate([s[0:1] for s in spare], axis=1)
    rest = jnp.concatenate([s[1:2] for s in spare], axis=1)
    return total + diag * (own - blocks[0][...].astype(F32)) + rest * own


def row_sum(block):
    return jnp.sum(block, axis=1, keepdims=True)


def first_kernel(pos_ref, *refs):
    grams, rs, (own_ref, w_ref, wb_ref, all_ref) = refs[:8], refs[8:16], refs[16:]
    w = product(pos_ref, grams, rs, own_ref[...], all_ref)
    w_ref[...] = w
    wb_ref[...] = w.astype(BF16)


def second_kernel(pos_ref, *refs):
    grams, rs, ws = refs[:8], refs[8:16], refs[16:24]
    r_ref, w_ref, z_ref, r1_ref, w1_ref, w1b_ref, scal_ref, all_ref = refs[24:]
    r0, w0 = r_ref[...], w_ref[...]
    z0 = product(pos_ref, grams, ws, w0, all_ref)
    norm = jnp.zeros(r0.shape, F32)
    curve = jnp.zeros(r0.shape, F32)
    for a, b in zip(rs, ws):
        r, w = a[...].astype(F32), b[...].astype(F32)
        norm += r * r
        curve += r * w
    norm0, curve0 = row_sum(norm), row_sum(curve)
    step0 = norm0 / curve0
    w1 = w0 - step0 * z0
    z_ref[...] = z0
    r1_ref[...] = r0 - step0 * w0
    w1_ref[...] = w1
    w1b_ref[...] = w1.astype(BF16)
    scal_ref[0] = wide(norm0)
    scal_ref[1] = wide(step0)


def third_kernel(pos_ref, *refs):
    grams, rs, ws, vs = refs[:8], refs[8:16], refs[16:24], refs[24:32]
    r_ref, w_ref, z_ref, r1_ref, w1_ref, scal_ref, x_ref, p_ref, out_ref, all_ref = refs[32:]
    r0, w0, z0, r1, w1 = (ref[...] for ref in (r_ref, w_ref, z_ref, r1_ref, w1_ref))
    norm0, step0 = scal_ref[0][:, :1], scal_ref[1][:, :1]
    q1 = product(pos_ref, grams, vs, w1, all_ref)
    norm = jnp.zeros(r0.shape, F32)
    curve = jnp.zeros(r0.shape, F32)
    for a, b, c in zip(rs, ws, vs):
        r = a[...].astype(F32) - step0 * b[...].astype(F32)
        norm += r * r
        curve += r * c[...].astype(F32)
    norm1 = row_sum(norm)
    beta1 = norm1 / norm0
    step1 = norm1 / (row_sum(curve) - beta1 * norm1 / step0)
    s1 = w1 + beta1 * w0
    z1 = q1 + beta1 * z0
    p1 = r1 + beta1 * r0
    r2 = r1 - step1 * s1
    w2 = w1 - step1 * z1
    norm = jnp.zeros(r0.shape, F32)
    for a, b, c in zip(rs, ws, vs):
        w = b[...].astype(F32)
        r = a[...].astype(F32) - step0 * w
        r = r - step1 * (c[...].astype(F32) + beta1 * w)
        norm += r * r
    norm2 = row_sum(norm)
    beta2 = norm2 / norm1
    x_ref[...] = step0 * r0 + step1 * p1
    p_ref[...] = r2 + beta2 * p1
    out_ref[0] = wide(norm2)
    out_ref[1] = wide(beta2 * norm2 / step1)
    out_ref[2] = wide(row_sum(r2 * w2))


def run(kernel, name, outs, pos, *args):
    shape = lambda kind: jax.ShapeDtypeStruct((COLS, CHUNK), kind)
    outs = [shape(o) if not isinstance(o, int) else jax.ShapeDtypeStruct((o, COLS, 128), F32) for o in outs]
    return pl.pallas_call(
        kernel,
        in_specs=[SMEM] + [VMEM] * len(args),
        out_specs=[VMEM] * len(outs),
        out_shape=outs,
        scratch_shapes=[pltpu.VMEM((16, COLS, ROWS), BF16)],
        cost_estimate=cost(2 * COLS * CHUNK * 4096, 4096 * CHUNK * 2),
        name=name,
    )(pos, *args)


def to_output(block):
    index = lambda y, core, z, x: ((y * 2 + core) * 4 + z) * 4 + x
    places = [(y, c, z, x) for y in range(4) for c in range(2) for z in range(4) for x in range(4)]
    odd = lax.axis_index("x") % 2
    halves = [block[:, :ROWS], block[:, ROWS:]]
    came = []
    for a in range(2):
        pairs = [
            (index(y, c, z, x), index(z, x // 2, y, 2 * c + ((x % 2) ^ a))) for y, c, z, x in places
        ]
        sent = jnp.where(odd == a, halves[0], halves[1])
        came.append(lax.ppermute(sent, ALL, pairs))
    first = jnp.where(odd == 0, came[0], came[1])
    second = jnp.where(odd == 0, came[1], came[0])
    return jnp.concatenate([first, second], axis=0).T


def shards(member_grams, member_weights):
    place = lax.axis_index(SHARD)
    chunk = lax.axis_index(MEMBER)
    pos = [lax.axis_index("y"), lax.axis_index("core"), 0, place, chunk, lax.axis_index("z"), lax.axis_index("x"), 0]
    pos = jnp.stack([jnp.asarray(p, jnp.int32) for p in pos])

    pieces = transposed(member_weights[0])
    grams = exchange(spread_grams(pos, member_grams[0]), MEMBER)
    early = gather_weights(pieces[0])
    late, grams = lax.optimization_barrier((pieces[1], grams))
    late = gather_weights(late)
    gram_sum = gather_grams(sum_grams(pos, grams))
    parts = []
    for piece, blocks in zip(PIECES, (early, late)):
        part = right_side_part(pos, grams, blocks).reshape(16, piece, CHUNK)
        parts.append(jnp.sum(exchange(part, SHARD).astype(F32), axis=0))
    r0 = jnp.concatenate(parts, axis=0)

    r0_all = gather(r0.astype(BF16))
    w0, w0_low = run(first_kernel, "product_0", (F32, BF16), pos, *gram_sum, *r0_all, r0)
    w0_all = gather(w0_low)
    z0, r1, w1, w1_low, scal = run(
        second_kernel, "product_1", (F32, F32, F32, BF16, 2), pos, *gram_sum, *r0_all, *w0_all, r0, w0
    )
    w1_all = gather(w1_low)
    x1, p2, last = run(
        third_kernel, "product_2", (F32, F32, 3), pos, *gram_sum, *r0_all, *w0_all, *w1_all, r0, w0, z0, r1, w1, scal
    )
    norm2, cross, curve = last[0, :, :1], last[1, :, :1], last[2, :, 0]
    curve = jnp.sum(exchange(jnp.broadcast_to(curve, (8, 1, COLS)), MEMBER), axis=(0, 1))[:, None]
    step2 = norm2 / (curve - cross)
    return to_output(x1 + step2 * p2)


def solution(mesh):
    fine = Mesh(mesh.devices.reshape(SIZES), ALL)
    return jax.shard_map(
        shards,
        mesh=fine,
        in_specs=(P(MEMBER, SHARD, None), P(MEMBER, SHARD, None)),
        out_specs=P(SHARD, MEMBER),
        check_vma=False,
    )
```

```python
import jax
import jax.numpy as jnp
from jax import lax
from jax.experimental import pallas as pl
from jax.experimental.pallas import tpu as pltpu
from jax.sharding import Mesh, PartitionSpec as P

MEMBER = ("y", "core")
SHARD = ("z", "x")
ALL = ("y", "core", "z", "x")
SIZES = (4, 2, 4, 4)
SHRINK = 0.9
ROWS = 256
CHUNK = 512
COLS = 144
PIECES = (64, 80)
SPARE = 16
FULL = ROWS + SPARE
F32 = jnp.float32
BF16 = jnp.bfloat16
VMEM = pl.BlockSpec(memory_space=pltpu.VMEM)
SMEM = pl.BlockSpec(memory_space=pltpu.SMEM)
HBM = pl.BlockSpec(memory_space=pltpu.HBM)
LIMIT = pltpu.CompilerParams(vmem_limit_bytes=16 * 2**20)


def exchange(parts, axis):
    return lax.all_to_all(parts, axis, split_axis=0, concat_axis=0, tiled=True)


def turn(block, axis, step):
    size = lax.axis_size(axis)
    return lax.ppermute(block, axis, [(i, (i + step) % size) for i in range(size)])


def dot(a, b):
    return jnp.dot(a, b, preferred_element_type=F32)


def cost(flops, moved):
    return pl.CostEstimate(flops=flops, bytes_accessed=moved, transcendentals=0)


def spare_rows(first, second):
    index = lax.broadcasted_iota(jnp.int32, (SPARE, first.shape[-1]), 0)
    return jnp.where(index == 0, first, jnp.where(index == 1, second, 0.0)).astype(BF16)


def transposed(weights):
    blocks = weights.shape[1] // COLS
    group = 8

    def body(w_ref, *out_refs):
        turned = w_ref[...].astype(F32).T.astype(BF16)
        for b in range(group):
            at = b * COLS
            for out_ref, piece in zip(out_refs, PIECES):
                out_ref[b * piece : (b + 1) * piece] = turned[at : at + piece]
                at += piece

    return pl.pallas_call(
        body,
        grid=(blocks // group,),
        in_specs=[pl.BlockSpec((ROWS, group * COLS), lambda i: (0, i))],
        out_specs=[pl.BlockSpec((group * p, ROWS), lambda i: (i, 0)) for p in PIECES],
        out_shape=[jax.ShapeDtypeStruct((blocks * p, ROWS), BF16) for p in PIECES],
        cost_estimate=cost(10**8, 2 * weights.size * 2),
        name="turn_weights",
    )(weights)


def spread_kernel(pos_ref, gram_ref, out_ref):
    for c in range(out_ref.shape[0]):
        gram = gram_ref[:, c * CHUNK : (c + 1) * CHUNK]
        first = (pl.program_id(0) * out_ref.shape[0] + c) * CHUNK
        row = lax.broadcasted_iota(jnp.int32, gram.shape, 0) + pos_ref[3] * ROWS
        col = lax.broadcasted_iota(jnp.int32, gram.shape, 1) + first
        on = row == col
        regular = jnp.where(on, gram, SHRINK * gram)
        low = regular.astype(BF16)
        rest = jnp.sum(jnp.where(on, regular - low.astype(F32), 0.0), axis=0, keepdims=True)
        out_ref[c, :ROWS] = low
        out_ref[c, ROWS:] = spare_rows(rest, jnp.zeros_like(rest))


def spread_grams(pos, gram):
    chunks = gram.shape[1] // CHUNK
    return pl.pallas_call(
        spread_kernel,
        grid=(chunks // 2,),
        in_specs=[SMEM, pl.BlockSpec((ROWS, 2 * CHUNK), lambda i: (0, i))],
        out_specs=pl.BlockSpec((2, FULL, CHUNK), lambda i: (i, 0, 0)),
        out_shape=jax.ShapeDtypeStruct((chunks, FULL, CHUNK), BF16),
        compiler_params=LIMIT,
        cost_estimate=cost(10**8, gram.size * 6),
        name="spread_grams",
    )(pos, gram)


def sum_kernel(pos_ref, blocks_ref, out_ref):
    total = jnp.sum(blocks_ref[...].astype(F32), axis=0)
    block, rest = total[:ROWS], total[ROWS : ROWS + 1]
    row = lax.broadcasted_iota(jnp.int32, block.shape, 0) + pos_ref[3] * ROWS
    col = lax.broadcasted_iota(jnp.int32, block.shape, 1) + pos_ref[4] * CHUNK
    on = row == col
    low = block.astype(BF16)
    kept = low.astype(F32)
    diag = jnp.sum(jnp.where(on, kept, 0.0), axis=0, keepdims=True)
    rest = rest + jnp.sum(jnp.where(on, block - kept, 0.0), axis=0, keepdims=True)
    out_ref[:ROWS] = low
    out_ref[ROWS:] = spare_rows(diag, rest)


def sum_grams(pos, blocks):
    return pl.pallas_call(
        sum_kernel,
        in_specs=[SMEM, VMEM],
        out_specs=VMEM,
        out_shape=jax.ShapeDtypeStruct((FULL, CHUNK), BF16),
        compiler_params=LIMIT,
        cost_estimate=cost(10**8, blocks.size * 2),
        name="sum_grams",
    )(pos, blocks)


def gather_weights(piece):
    middle = piece.shape[0] // 2
    up, down = turn(piece, "y", 1), turn(piece, "y", 3)
    far = [turn(up[:middle], "y", 1), turn(down[middle:], "y", 3)]
    mine = [piece, up, down] + far
    return mine + [turn(b, "core", 1) for b in mine]


def right_side_kernel(pos_ref, g_ref, *refs):
    blocks, out_ref = refs[:-1], refs[-1]
    y, core = pos_ref[0], pos_ref[1]
    grams = []
    for other in range(2):
        for step in (0, 3, 1, 2):
            grams.append(g_ref.at[2 * lax.rem(y + step, 4) + (1 - core if other else core)])
    middle = out_ref.shape[0] // 2
    for part in range(2):
        rows = slice(part * middle, (part + 1) * middle)
        total = jnp.zeros((middle, out_ref.shape[1]), F32)
        for other in range(2):
            five = blocks[5 * other : 5 * other + 5]
            for k in range(3):
                total += dot(five[k][rows], grams[4 * other + k][:ROWS])
            total += dot(five[3 + part][...], grams[4 * other + 3][:ROWS])
        out_ref[rows] = total.astype(BF16)


def right_side_part(pos, grams, blocks):
    rows = blocks[0].shape[0]
    return pl.pallas_call(
        right_side_kernel,
        in_specs=[SMEM, VMEM] + [VMEM] * len(blocks),
        out_specs=VMEM,
        out_shape=jax.ShapeDtypeStruct((rows, CHUNK), BF16),
        compiler_params=LIMIT,
        cost_estimate=cost(2 * rows * CHUNK * ROWS * 8, rows * ROWS * 16 + grams.size * 2 + rows * CHUNK * 2),
        name="right_side",
    )(pos, grams, *blocks)


def gather(block):
    mine = [block] + [turn(block, "y", step) for step in (1, 2, 3)]
    return mine + [turn(b, "core", 1) for b in mine]


def fetch(pos_ref, gram_hbm, parts, gram_ref, all_ref, sems):
    y, core = pos_ref[0], pos_ref[1]
    copies = []
    for i, part in enumerate(parts):
        at = lax.rem(y + 4 - i % 4, 4) * 2 + (core if i < 4 else 1 - core)
        copies.append(pltpu.make_async_copy(part, all_ref.at[at], sems.at[i]))
    grams = []
    for i in range(4):
        some = pl.ds(4 * i, 4)
        grams.append(pltpu.make_async_copy(gram_hbm.at[some], gram_ref.at[some], sems.at[8 + i]))
    for copy in copies + grams:
        copy.start()
    for copy in copies:
        copy.wait()
    return 2 * y + core, grams


def product(gram_ref, all_ref, at, grams, own):
    total = jnp.zeros(own.shape, F32)
    spare = jnp.zeros((8, CHUNK), F32)
    for s in range(16):
        if s % 4 == 0:
            grams[s // 4].wait()
        h = s % 2
        total += dot(all_ref[s // 2, :COLS, h * ROWS : (h + 1) * ROWS], gram_ref[s, :ROWS])
        spare += gram_ref[s, ROWS:].astype(F32)[:8]
    return total + spare[0:1] * (own - all_ref[at, :COLS].astype(F32)) + spare[1:2] * own


def own_sum(a, b):
    ones = jnp.ones((8, CHUNK), F32)
    return lax.dot_general(
        ones, a * b, (((1,), (1,)), ((), ())), precision=lax.Precision.HIGHEST, preferred_element_type=F32
    )


def put(out_ref, block, first, second):
    out_ref[:COLS] = block.astype(BF16)
    index = lax.broadcasted_iota(jnp.int32, (16, COLS), 0)
    rows = jnp.zeros((16, COLS), F32)
    for i, own in enumerate((first, second)):
        left = own[0:1]
        for j in range(3):
            top = left.astype(BF16).astype(F32)
            rows = jnp.where(index == 3 * i + j, top, rows)
            left = left - top
    out_ref[COLS:] = jnp.concatenate([rows, jnp.zeros((16, CHUNK - COLS), F32)], axis=1).astype(BF16)


def take(all_ref):
    rows = jnp.sum(all_ref[:, COLS:].astype(F32), axis=0)
    out = []
    for i in range(2):
        row = rows[3 * i : 3 * i + 1] + (rows[3 * i + 1 : 3 * i + 2] + rows[3 * i + 2 : 3 * i + 3])
        out.append(jnp.broadcast_to(row[:, :256], (128, 256)).T[:COLS, :1])
    return out


def wide(column):
    return jnp.broadcast_to(column, (column.shape[0], 128))


def first_kernel(times, sums, own_refs, outs):
    r0 = own_refs[0][...]
    w_ref, send_ref = outs
    w0 = times(r0)
    w_ref[...] = w0
    put(send_ref, w0, own_sum(r0, r0), own_sum(r0, w0))


def second_kernel(times, sums, own_refs, outs):
    r0, w0 = (ref[...] for ref in own_refs)
    z_ref, r1_ref, w1_ref, send_ref = outs
    norm0, curve0 = sums()
    step0 = norm0 / curve0
    z0 = times(w0)
    r1 = r0 - step0 * w0
    w1 = w0 - step0 * z0
    z_ref[:, :CHUNK] = z0
    z_ref[:, CHUNK : CHUNK + 128] = wide(norm0)
    z_ref[:, CHUNK + 128 :] = wide(step0)
    r1_ref[...] = r1
    w1_ref[...] = w1
    put(send_ref, w1, own_sum(r1, r1), own_sum(r1, w1))


def third_kernel(times, sums, own_refs, outs):
    r0, w0, z0, r1, w1 = (ref[...] for ref in own_refs)
    x_ref, r2_ref, p_ref, sums_ref = outs
    norm0, step0 = z0[:, CHUNK : CHUNK + 1], z0[:, CHUNK + 128 : CHUNK + 129]
    z0 = z0[:, :CHUNK]
    norm1, curve1 = sums()
    beta1 = norm1 / norm0
    step1 = norm1 / (curve1 - beta1 * norm1 / step0)
    p1 = r1 + beta1 * r0
    r2 = r1 - step1 * (w1 + beta1 * w0)
    x_ref[...] = step0 * r0 + step1 * p1
    r2_ref[...] = r2
    p_ref[:, :CHUNK] = p1
    p_ref[:, CHUNK : CHUNK + 128] = wide(norm1)
    p_ref[:, CHUNK + 128 :] = wide(step1)
    norm2 = own_sum(r2, r2)
    w2 = w1 - step1 * (times(w1) + beta1 * z0)
    sums_ref[...] = jnp.concatenate([norm2, own_sum(r2, w2)], axis=1)


def run(body, outs, gram_sum, parts, pos, *owns):
    rows = parts[0].shape[0]

    def kernel(pos_ref, *refs):
        own_refs, gram_hbm, part_refs = refs[: len(owns)], refs[len(owns)], refs[len(owns) + 1 : len(owns) + 9]
        out_refs, (gram_ref, all_ref, sems) = refs[len(owns) + 9 : -3], refs[-3:]
        at, grams = fetch(pos_ref, gram_hbm, part_refs, gram_ref, all_ref, sems)
        body(lambda own: product(gram_ref, all_ref, at, grams, own), lambda: take(all_ref), own_refs, out_refs)

    return pl.pallas_call(
        kernel,
        in_specs=[SMEM] + [VMEM] * len(owns) + [HBM] * (1 + len(parts)),
        out_specs=[VMEM] * len(outs),
        out_shape=outs,
        scratch_shapes=[
            pltpu.VMEM(gram_sum.shape, BF16),
            pltpu.VMEM((8, rows, CHUNK), BF16),
            pltpu.SemaphoreType.DMA((12,)),
        ],
        compiler_params=LIMIT,
        cost_estimate=cost(2 * COLS * CHUNK * 4096, 4096 * CHUNK * 2),
    )(pos, *owns, gram_sum, *parts)


def to_output(block):
    index = lambda y, core, z, x: ((y * 2 + core) * 4 + z) * 4 + x
    places = [(y, c, z, x) for y in range(4) for c in range(2) for z in range(4) for x in range(4)]
    odd = lax.axis_index("x") % 2
    halves = [block[:, :ROWS], block[:, ROWS:]]
    came = []
    for a in range(2):
        pairs = [
            (index(y, c, z, x), index(z, x // 2, y, 2 * c + ((x % 2) ^ a))) for y, c, z, x in places
        ]
        sent = jnp.where(odd == a, halves[0], halves[1])
        came.append(lax.ppermute(sent, ALL, pairs))
    first = jnp.where(odd == 0, came[0], came[1])
    second = jnp.where(odd == 0, came[1], came[0])
    return jnp.concatenate([first, second], axis=0).T


def shards(member_grams, member_weights):
    place = lax.axis_index(SHARD)
    chunk = lax.axis_index(MEMBER)
    pos = [lax.axis_index("y"), lax.axis_index("core"), 0, place, chunk, lax.axis_index("z"), lax.axis_index("x"), 0]
    pos = jnp.stack([jnp.asarray(p, jnp.int32) for p in pos])

    pieces = transposed(member_weights[0])
    early = gather_weights(pieces[0])
    ready, pieces = lax.optimization_barrier((pos, pieces))
    spread = spread_grams(ready, member_grams[0])
    grams = exchange(spread, MEMBER)
    late, grams = lax.optimization_barrier((pieces[1], grams))
    late = gather_weights(late)
    gram_sum = lax.all_gather(sum_grams(pos, grams), SHARD, axis=0)
    parts = []
    for piece, blocks in zip(PIECES, (early, late)):
        part = right_side_part(pos, grams, blocks)
        part = exchange(part.reshape(16, piece, CHUNK), SHARD)
        parts.append(jnp.sum(part.astype(F32), axis=0))
    r0 = jnp.concatenate(parts, axis=0)

    array = jax.ShapeDtypeStruct((COLS, CHUNK), F32)
    more = jax.ShapeDtypeStruct((COLS, CHUNK + 256), F32)
    sent = jax.ShapeDtypeStruct((COLS + 16, CHUNK), BF16)
    sums = jax.ShapeDtypeStruct((8, 2 * COLS), F32)
    w0, low = run(first_kernel, (array, sent), gram_sum, gather(r0.astype(BF16)), pos, r0)
    outs = (more, array, array, sent)
    z0, r1, w1, low = run(second_kernel, outs, gram_sum, gather(low), pos, r0, w0)
    outs = (array, array, more, sums)
    x1, r2, p1, both = run(third_kernel, outs, gram_sum, gather(low), pos, r0, w0, z0, r1, w1)
    norm1, step1 = p1[:, CHUNK : CHUNK + 1], p1[:, CHUNK + 128 : CHUNK + 129]
    p1 = p1[:, :CHUNK]
    both = jnp.sum(exchange(both.reshape(8, 1, 2 * COLS), MEMBER), axis=(0, 1))
    norm2, curve2 = both[:COLS, None], both[COLS:, None]
    beta2 = norm2 / norm1
    step2 = norm2 / (curve2 - beta2 * norm2 / step1)
    p2 = r2 + beta2 * p1
    return to_output(x1 + step2 * p2)


def solution(mesh):
    fine = Mesh(mesh.devices.reshape(SIZES), ALL)

    return jax.shard_map(
        shards,
        mesh=fine,
        in_specs=(P(MEMBER, SHARD, None), P(MEMBER, SHARD, None)),
        out_specs=P(SHARD, MEMBER),
        check_vma=False,
    )
```

```python
import jax
import jax.numpy as jnp
from jax import lax
from jax.experimental import pallas as pl
from jax.experimental.pallas import tpu as pltpu
from jax.sharding import Mesh, PartitionSpec as P

MEMBER = ("y", "core")
SHARD = ("z", "x")
ALL = ("y", "core", "z", "x")
SIZES = (4, 2, 4, 4)
SHRINK = 0.9
ROWS = 256
CHUNK = 512
COLS = 144
PIECES = (64, 80)
SPARE = 16
FULL = ROWS + SPARE
F32 = jnp.float32
BF16 = jnp.bfloat16
VMEM = pl.BlockSpec(memory_space=pltpu.VMEM)
SMEM = pl.BlockSpec(memory_space=pltpu.SMEM)
HBM = pl.BlockSpec(memory_space=pltpu.HBM)
LIMIT = pltpu.CompilerParams(vmem_limit_bytes=16 * 2**20)


def exchange(parts, axis):
    return lax.all_to_all(parts, axis, split_axis=0, concat_axis=0, tiled=True)


def turn(block, axis, step):
    size = lax.axis_size(axis)
    return lax.ppermute(block, axis, [(i, (i + step) % size) for i in range(size)])


def dot(a, b):
    return jnp.dot(a, b, preferred_element_type=F32)


def cost(flops, moved):
    return pl.CostEstimate(flops=flops, bytes_accessed=moved, transcendentals=0)


def spare_rows(first, second):
    index = lax.broadcasted_iota(jnp.int32, (SPARE, first.shape[-1]), 0)
    return jnp.where(index == 0, first, jnp.where(index == 1, second, 0.0)).astype(BF16)


def transposed(weights):
    blocks = weights.shape[1] // COLS
    group = 8

    def body(w_ref, *out_refs):
        turned = w_ref[...].astype(F32).T.astype(BF16)
        for b in range(group):
            at = b * COLS
            for out_ref, piece in zip(out_refs, PIECES):
                out_ref[b * piece : (b + 1) * piece] = turned[at : at + piece]
                at += piece

    return pl.pallas_call(
        body,
        grid=(blocks // group,),
        in_specs=[pl.BlockSpec((ROWS, group * COLS), lambda i: (0, i))],
        out_specs=[pl.BlockSpec((group * p, ROWS), lambda i: (i, 0)) for p in PIECES],
        out_shape=[jax.ShapeDtypeStruct((blocks * p, ROWS), BF16) for p in PIECES],
        cost_estimate=cost(10**8, 2 * weights.size * 2),
        name="turn_weights",
    )(weights)


def spread_kernel(pos_ref, gram_ref, out_ref):
    for c in range(out_ref.shape[0]):
        gram = gram_ref[:, c * CHUNK : (c + 1) * CHUNK]
        first = (pl.program_id(0) * out_ref.shape[0] + c) * CHUNK
        row = lax.broadcasted_iota(jnp.int32, gram.shape, 0) + pos_ref[3] * ROWS
        col = lax.broadcasted_iota(jnp.int32, gram.shape, 1) + first
        on = row == col
        regular = jnp.where(on, gram, SHRINK * gram)
        low = regular.astype(BF16)
        rest = jnp.sum(jnp.where(on, regular - low.astype(F32), 0.0), axis=0, keepdims=True)
        out_ref[c, :ROWS] = low
        out_ref[c, ROWS:] = spare_rows(rest, jnp.zeros_like(rest))


def spread_grams(pos, gram):
    chunks = gram.shape[1] // CHUNK
    return pl.pallas_call(
        spread_kernel,
        grid=(chunks // 2,),
        in_specs=[SMEM, pl.BlockSpec((ROWS, 2 * CHUNK), lambda i: (0, i))],
        out_specs=pl.BlockSpec((2, FULL, CHUNK), lambda i: (i, 0, 0)),
        out_shape=jax.ShapeDtypeStruct((chunks, FULL, CHUNK), BF16),
        cost_estimate=cost(10**8, gram.size * 6),
        name="spread_grams",
    )(pos, gram)


def sum_kernel(pos_ref, blocks_ref, *out_refs):
    total = jnp.sum(blocks_ref[...].astype(F32), axis=0)
    block, rest = total[:ROWS], total[ROWS : ROWS + 1]
    row = lax.broadcasted_iota(jnp.int32, block.shape, 0) + pos_ref[3] * ROWS
    col = lax.broadcasted_iota(jnp.int32, block.shape, 1) + pos_ref[4] * CHUNK
    on = row == col
    low = block.astype(BF16)
    kept = low.astype(F32)
    diag = jnp.sum(jnp.where(on, kept, 0.0), axis=0, keepdims=True)
    rest = rest + jnp.sum(jnp.where(on, block - kept, 0.0), axis=0, keepdims=True)
    spare = spare_rows(diag, rest)
    half = CHUNK // 2
    for h, out_ref in enumerate(out_refs):
        out_ref[:ROWS] = low[:, h * half : (h + 1) * half]
        out_ref[ROWS:] = spare[:, h * half : (h + 1) * half]


def sum_grams(pos, blocks):
    half = jax.ShapeDtypeStruct((FULL, CHUNK // 2), BF16)
    return pl.pallas_call(
        sum_kernel,
        in_specs=[SMEM, VMEM],
        out_specs=[VMEM, VMEM],
        out_shape=[half, half],
        compiler_params=LIMIT,
        cost_estimate=cost(10**8, blocks.size * 2),
        name="sum_grams",
    )(pos, blocks)


def gather_line(half, axis):
    return jnp.stack([half] + [turn(half, axis, step) for step in (1, 2, 3)])


def gather_plane(lines):
    out = []
    for line, axis in zip(lines, ("z", "x")):
        out += [line] + [turn(line, axis, step) for step in (1, 2, 3)]
    return out


def gather_weights(piece):
    middle = piece.shape[0] // 2
    up, down = turn(piece, "y", 1), turn(piece, "y", 3)
    far = [turn(up[:middle], "y", 1), turn(down[middle:], "y", 3)]
    others = [turn(b, "core", 1) for b in (piece, up, down)]
    others += [turn(b, "core", 1) for b in far]
    return [piece, up, down] + far + others


def right_side_kernel(pos_ref, g_ref, *refs):
    blocks, out_ref = refs[:-1], refs[-1]
    y, core = pos_ref[0], pos_ref[1]
    grams = []
    for other in range(2):
        for step in (0, 3, 1, 2):
            grams.append(g_ref.at[2 * lax.rem(y + step, 4) + (1 - core if other else core)])
    middle = out_ref.shape[0] // 2
    for part in range(2):
        rows = slice(part * middle, (part + 1) * middle)
        total = jnp.zeros((middle, out_ref.shape[1]), F32)
        for other in range(2):
            five = blocks[5 * other : 5 * other + 5]
            for k in range(3):
                total += dot(five[k][rows], grams[4 * other + k][:ROWS])
            total += dot(five[3 + part][...], grams[4 * other + 3][:ROWS])
        out_ref[rows] = total.astype(BF16)


def right_side_part(pos, grams, blocks):
    rows = blocks[0].shape[0]
    return pl.pallas_call(
        right_side_kernel,
        in_specs=[SMEM, VMEM] + [VMEM] * len(blocks),
        out_specs=VMEM,
        out_shape=jax.ShapeDtypeStruct((rows, CHUNK), BF16),
        compiler_params=LIMIT,
        cost_estimate=cost(2 * rows * CHUNK * ROWS * 8, rows * ROWS * 16 + grams.size * 2 + rows * CHUNK * 2),
        name="right_side",
    )(pos, grams, *blocks)


def gather(block):
    mine = [block] + [turn(block, "y", step) for step in (1, 2, 3)]
    return mine + [turn(b, "core", 1) for b in mine]


def fetch(pos_ref, parts, all_ref, sems):
    y, core = pos_ref[0], pos_ref[1]
    copies = []
    for i, part in enumerate(parts):
        at = lax.rem(y + 4 - i % 4, 4) * 2 + (core if i < 4 else 1 - core)
        copies.append(pltpu.make_async_copy(part, all_ref.at[at], sems.at[i]))
    for copy in copies:
        copy.start()
    for copy in copies:
        copy.wait()
    return 2 * y + core


def product(pos_ref, gram_refs, all_ref, at, own):
    z, x = pos_ref[5], pos_ref[6]
    sums = []
    spare = []
    for half in range(2):
        total = jnp.zeros((own.shape[0], CHUNK // 2), F32)
        extra = jnp.zeros((8, CHUNK // 2), F32)
        for a in range(4):
            for b in range(4):
                k, j = (a, b) if half == 0 else (b, a)
                j = lax.rem(x + 4 - j, 4)
                chunk = 2 * lax.rem(z + 4 - k, 4) + lax.div(j, 2)
                lanes = pl.ds(pl.multiple_of(lax.rem(j, 2) * ROWS, ROWS), ROWS)
                ref = gram_refs[4 * half + a]
                total += dot(all_ref[chunk, : own.shape[0], lanes], ref[b, :ROWS])
                extra += ref[b, ROWS:].astype(F32)[:8]
        sums.append(total)
        spare.append(extra)
    total = jnp.concatenate(sums, axis=1)
    spare = jnp.concatenate(spare, axis=1)
    return total + spare[0:1] * (own - all_ref[at, : own.shape[0]].astype(F32)) + spare[1:2] * own


def own_sum(a, b):
    ones = jnp.ones((8, CHUNK), F32)
    return lax.dot_general(
        ones, a * b, (((1,), (1,)), ((), ())), precision=lax.Precision.HIGHEST, preferred_element_type=F32
    )


def put(out_ref, block, first, second):
    out_ref[:COLS] = block.astype(BF16)
    index = lax.broadcasted_iota(jnp.int32, (16, COLS), 0)
    rows = jnp.zeros((16, COLS), F32)
    for i, own in enumerate((first, second)):
        left = own[0:1]
        for j in range(3):
            top = left.astype(BF16).astype(F32)
            rows = jnp.where(index == 3 * i + j, top, rows)
            left = left - top
    out_ref[COLS:] = jnp.concatenate([rows, jnp.zeros((16, CHUNK - COLS), F32)], axis=1).astype(BF16)


def take(all_ref):
    rows = jnp.sum(all_ref[:, COLS:].astype(F32), axis=0)
    out = []
    for i in range(2):
        row = rows[3 * i : 3 * i + 1] + (rows[3 * i + 1 : 3 * i + 2] + rows[3 * i + 2 : 3 * i + 3])
        out.append(jnp.broadcast_to(row[:, :256], (128, 256)).T[:COLS, :1])
    return out


def wide(column):
    return jnp.broadcast_to(column, (column.shape[0], 128))


def first_kernel(times, sums, own_refs, outs):
    r0 = own_refs[0][...]
    w_ref, send_ref = outs
    w0 = times(r0)
    w_ref[...] = w0
    put(send_ref, w0, own_sum(r0, r0), own_sum(r0, w0))


def second_kernel(times, sums, own_refs, outs):
    r0, w0 = (ref[...] for ref in own_refs)
    z_ref, r1_ref, w1_ref, send_ref = outs
    norm0, curve0 = sums()
    step0 = norm0 / curve0
    z0 = times(w0)
    r1 = r0 - step0 * w0
    w1 = w0 - step0 * z0
    z_ref[:, :CHUNK] = z0
    z_ref[:, CHUNK : CHUNK + 128] = wide(norm0)
    z_ref[:, CHUNK + 128 :] = wide(step0)
    r1_ref[...] = r1
    w1_ref[...] = w1
    put(send_ref, w1, own_sum(r1, r1), own_sum(r1, w1))


def third_kernel(times, sums, own_refs, outs):
    r0, w0, z0, r1, w1 = (ref[...] for ref in own_refs)
    last_ref, sums_ref = outs
    norm0, step0 = z0[:, CHUNK : CHUNK + 1], z0[:, CHUNK + 128 : CHUNK + 129]
    z0 = z0[:, :CHUNK]
    norm1, curve1 = sums()
    beta1 = norm1 / norm0
    step1 = norm1 / (curve1 - beta1 * norm1 / step0)
    p1 = r1 + beta1 * r0
    r2 = r1 - step1 * (w1 + beta1 * w0)
    last_ref[:, :CHUNK] = step0 * r0 + step1 * p1
    last_ref[:, CHUNK : 2 * CHUNK] = r2
    last_ref[:, 2 * CHUNK : 3 * CHUNK] = p1
    last_ref[:, 3 * CHUNK : 3 * CHUNK + 128] = wide(norm1)
    last_ref[:, 3 * CHUNK + 128 :] = wide(step1)
    norm2 = own_sum(r2, r2)
    w2 = w1 - step1 * (times(w1) + beta1 * z0)
    sums_ref[:, 0, :] = jnp.concatenate([norm2, own_sum(r2, w2)], axis=1)


def run(body, outs, grams, parts, pos, *owns):
    rows = parts[0].shape[0]

    def kernel(pos_ref, *refs):
        groups = []
        for n in (len(owns), len(grams), len(parts), len(outs)):
            groups.append(refs[:n])
            refs = refs[n:]
        own_refs, gram_refs, part_refs, out_refs = groups
        all_ref, sems = refs
        at = fetch(pos_ref, part_refs, all_ref, sems)
        times = lambda own: product(pos_ref, gram_refs, all_ref, at, own)
        body(times, lambda: take(all_ref), own_refs, out_refs)

    return pl.pallas_call(
        kernel,
        in_specs=[SMEM] + [VMEM] * (len(owns) + len(grams)) + [HBM] * len(parts),
        out_specs=[VMEM] * len(outs),
        out_shape=outs,
        scratch_shapes=[pltpu.VMEM((8, rows, CHUNK), BF16), pltpu.SemaphoreType.DMA((8,))],
        compiler_params=LIMIT,
        cost_estimate=cost(2 * COLS * CHUNK * 4096, 4096 * CHUNK * 2),
    )(pos, *owns, *grams, *parts)


def to_output(block):
    index = lambda y, core, z, x: ((y * 2 + core) * 4 + z) * 4 + x
    places = [(y, c, z, x) for y in range(4) for c in range(2) for z in range(4) for x in range(4)]
    odd = lax.axis_index("x") % 2
    halves = [block[:, :ROWS], block[:, ROWS:]]
    came = []
    for a in range(2):
        pairs = [
            (index(y, c, z, x), index(z, x // 2, y, 2 * c + ((x % 2) ^ a))) for y, c, z, x in places
        ]
        sent = jnp.where(odd == a, halves[0], halves[1])
        came.append(lax.ppermute(sent, ALL, pairs))
    first = jnp.where(odd == 0, came[0], came[1])
    second = jnp.where(odd == 0, came[1], came[0])
    return jnp.concatenate([first, second], axis=0).T


def shards(member_grams, member_weights):
    place = lax.axis_index(SHARD)
    chunk = lax.axis_index(MEMBER)
    pos = [lax.axis_index("y"), lax.axis_index("core"), 0, place, chunk, lax.axis_index("z"), lax.axis_index("x"), 0]
    pos = jnp.stack([jnp.asarray(p, jnp.int32) for p in pos])

    pieces = transposed(member_weights[0])
    early = gather_weights(pieces[0])
    ready, pieces = lax.optimization_barrier((pos, pieces))
    spread = spread_grams(ready, member_grams[0])
    grams = exchange(spread, MEMBER)
    late, grams = lax.optimization_barrier((pieces[1], grams))
    late = gather_weights(late)
    gram_sum = gather_plane([gather_line(half, axis) for half, axis in zip(sum_grams(pos, grams), ("x", "z"))])
    parts = []
    for piece, blocks in zip(PIECES, (early, late)):
        part = right_side_part(pos, grams, blocks)
        part = exchange(part.reshape(16, piece, CHUNK), SHARD)
        parts.append(jnp.sum(part.astype(F32), axis=0))
    r0 = jnp.concatenate(parts, axis=0)

    array = jax.ShapeDtypeStruct((COLS, CHUNK), F32)
    more = jax.ShapeDtypeStruct((COLS, CHUNK + 256), F32)
    sent = jax.ShapeDtypeStruct((COLS + 16, CHUNK), BF16)
    packed = jax.ShapeDtypeStruct((COLS, 3 * CHUNK + 256), F32)
    sums = jax.ShapeDtypeStruct((8, 1, 2 * COLS), F32)
    w0, low = run(first_kernel, (array, sent), gram_sum, gather(r0.astype(BF16)), pos, r0)
    outs = (more, array, array, sent)
    z0, r1, w1, low = run(second_kernel, outs, gram_sum, gather(low), pos, r0, w0)
    outs = (packed, sums)
    last, both = run(third_kernel, outs, gram_sum, gather(low), pos, r0, w0, z0, r1, w1)
    x1, r2, p1 = (last[:, i * CHUNK : (i + 1) * CHUNK] for i in range(3))
    norm1, step1 = last[:, 3 * CHUNK : 3 * CHUNK + 1], last[:, 3 * CHUNK + 128 : 3 * CHUNK + 129]
    both = sum(gather(both))[0, 0]
    norm2, curve2 = both[:COLS, None], both[COLS:, None]
    beta2 = norm2 / norm1
    step2 = norm2 / (curve2 - beta2 * norm2 / step1)
    p2 = r2 + beta2 * p1
    return to_output(x1 + step2 * p2)


def solution(mesh):
    fine = Mesh(mesh.devices.reshape(SIZES), ALL)

    return jax.shard_map(
        shards,
        mesh=fine,
        in_specs=(P(MEMBER, SHARD, None), P(MEMBER, SHARD, None)),
        out_specs=P(SHARD, MEMBER),
        check_vma=False,
    )
```

```python
import jax
import jax.numpy as jnp
from jax import lax
from jax.experimental import pallas as pl
from jax.experimental.pallas import tpu as pltpu
from jax.sharding import Mesh, PartitionSpec as P

MEMBER = ("y", "core")
SHARD = ("z", "x")
ALL = ("y", "core", "z", "x")
SIZES = (4, 2, 4, 4)
SHRINK = 0.9
ROWS = 256
CHUNK = 512
COLS = 144
PIECES = (64, 80)
SPARE = 16
FULL = ROWS + SPARE
F32 = jnp.float32
BF16 = jnp.bfloat16
VMEM = pl.BlockSpec(memory_space=pltpu.VMEM)
SMEM = pl.BlockSpec(memory_space=pltpu.SMEM)
HBM = pl.BlockSpec(memory_space=pltpu.HBM)
LIMIT = pltpu.CompilerParams(vmem_limit_bytes=16 * 2**20)


def exchange(parts, axis):
    return lax.all_to_all(parts, axis, split_axis=0, concat_axis=0, tiled=True)


def turn(block, axis, step):
    size = lax.axis_size(axis)
    return lax.ppermute(block, axis, [(i, (i + step) % size) for i in range(size)])


def dot(a, b):
    return jnp.dot(a, b, preferred_element_type=F32)


def cost(flops, moved):
    return pl.CostEstimate(flops=flops, bytes_accessed=moved, transcendentals=0)


def spare_rows(first, second):
    index = lax.broadcasted_iota(jnp.int32, (SPARE, first.shape[-1]), 0)
    return jnp.where(index == 0, first, jnp.where(index == 1, second, 0.0)).astype(BF16)


def transposed(weights):
    blocks = weights.shape[1] // COLS
    group = 8

    def body(w_ref, *out_refs):
        turned = w_ref[...].astype(F32).T.astype(BF16)
        for b in range(group):
            at = b * COLS
            for out_ref, piece in zip(out_refs, PIECES):
                out_ref[b * piece : (b + 1) * piece] = turned[at : at + piece]
                at += piece

    return pl.pallas_call(
        body,
        grid=(blocks // group,),
        in_specs=[pl.BlockSpec((ROWS, group * COLS), lambda i: (0, i))],
        out_specs=[pl.BlockSpec((group * p, ROWS), lambda i: (i, 0)) for p in PIECES],
        out_shape=[jax.ShapeDtypeStruct((blocks * p, ROWS), BF16) for p in PIECES],
        cost_estimate=cost(10**8, 2 * weights.size * 2),
        name="turn_weights",
    )(weights)


def spread_kernel(pos_ref, gram_ref, out_ref):
    for c in range(out_ref.shape[0]):
        gram = gram_ref[:, c * CHUNK : (c + 1) * CHUNK]
        first = (pl.program_id(0) * out_ref.shape[0] + c) * CHUNK
        row = lax.broadcasted_iota(jnp.int32, gram.shape, 0) + pos_ref[3] * ROWS
        col = lax.broadcasted_iota(jnp.int32, gram.shape, 1) + first
        on = row == col
        regular = jnp.where(on, gram, SHRINK * gram)
        low = regular.astype(BF16)
        rest = jnp.sum(jnp.where(on, regular - low.astype(F32), 0.0), axis=0, keepdims=True)
        out_ref[c, :ROWS] = low
        out_ref[c, ROWS:] = spare_rows(rest, jnp.zeros_like(rest))


def spread_grams(pos, gram):
    chunks = gram.shape[1] // CHUNK
    return pl.pallas_call(
        spread_kernel,
        grid=(chunks // 2,),
        in_specs=[SMEM, pl.BlockSpec((ROWS, 2 * CHUNK), lambda i: (0, i))],
        out_specs=pl.BlockSpec((2, FULL, CHUNK), lambda i: (i, 0, 0)),
        out_shape=jax.ShapeDtypeStruct((chunks, FULL, CHUNK), BF16),
        cost_estimate=cost(10**8, gram.size * 6),
        name="spread_grams",
    )(pos, gram)


def sum_kernel(pos_ref, blocks_ref, *out_refs):
    total = jnp.sum(blocks_ref[...].astype(F32), axis=0)
    block, rest = total[:ROWS], total[ROWS : ROWS + 1]
    row = lax.broadcasted_iota(jnp.int32, block.shape, 0) + pos_ref[3] * ROWS
    col = lax.broadcasted_iota(jnp.int32, block.shape, 1) + pos_ref[4] * CHUNK
    on = row == col
    low = block.astype(BF16)
    kept = low.astype(F32)
    diag = jnp.sum(jnp.where(on, kept, 0.0), axis=0, keepdims=True)
    rest = rest + jnp.sum(jnp.where(on, block - kept, 0.0), axis=0, keepdims=True)
    spare = spare_rows(diag, rest)
    half = CHUNK // 2
    for h, out_ref in enumerate(out_refs):
        out_ref[:ROWS] = low[:, h * half : (h + 1) * half]
        out_ref[ROWS:] = spare[:, h * half : (h + 1) * half]


def sum_grams(pos, blocks):
    half = jax.ShapeDtypeStruct((FULL, CHUNK // 2), BF16)
    return pl.pallas_call(
        sum_kernel,
        in_specs=[SMEM, VMEM],
        out_specs=[VMEM, VMEM],
        out_shape=[half, half],
        compiler_params=LIMIT,
        cost_estimate=cost(10**8, blocks.size * 2),
        name="sum_grams",
    )(pos, blocks)


def gather_line(half, axis):
    return jnp.stack([half] + [turn(half, axis, step) for step in (1, 2, 3)])


def gather_plane(lines):
    out = []
    for line, axis in zip(lines, ("z", "x")):
        out += [line] + [turn(line, axis, step) for step in (1, 2, 3)]
    return out


def gather_weights(piece, split):
    middle = piece.shape[0] // 2
    up, down = turn(piece, "y", 1), turn(piece, "y", 3)
    far = [turn(up[:middle], "y", 1), turn(down[middle:], "y", 3)] if split else [turn(down, "y", 3)]
    others = [turn(b, "core", 1) for b in (piece, up, down)]
    others += [turn(b, "core", 1) for b in far]
    return [piece, up, down] + far + others


def right_side_kernel(pos_ref, g_ref, *refs):
    blocks, out_ref = refs[:-1], refs[-1]
    y, core = pos_ref[0], pos_ref[1]
    grams = []
    for other in range(2):
        for step in (0, 3, 1, 2):
            grams.append(g_ref.at[2 * lax.rem(y + step, 4) + (1 - core if other else core)])
    middle = out_ref.shape[0] // 2
    for part in range(2):
        rows = slice(part * middle, (part + 1) * middle)
        total = jnp.zeros((middle, out_ref.shape[1]), F32)
        count = len(blocks) // 2
        for other in range(2):
            some = blocks[count * other : count * other + count]
            for k in range(3):
                total += dot(some[k][rows], grams[4 * other + k][:ROWS])
            far = some[3 + part][...] if count == 5 else some[3][rows]
            total += dot(far, grams[4 * other + 3][:ROWS])
        out_ref[rows] = total.astype(BF16)


def right_side_part(pos, grams, blocks):
    rows = blocks[0].shape[0]
    return pl.pallas_call(
        right_side_kernel,
        in_specs=[SMEM, VMEM] + [VMEM] * len(blocks),
        out_specs=VMEM,
        out_shape=jax.ShapeDtypeStruct((rows, CHUNK), BF16),
        compiler_params=LIMIT,
        cost_estimate=cost(2 * rows * CHUNK * ROWS * 8, rows * ROWS * 16 + grams.size * 2 + rows * CHUNK * 2),
        name="right_side",
    )(pos, grams, *blocks)


def gather(block):
    mine = [block]
    for step in (1, 2, 3):
        mine.append(turn(block, "y", step))
    return mine + [turn(b, "core", 1) for b in mine]


def fetch(pos_ref, parts, all_ref, sems):
    y, core = pos_ref[0], pos_ref[1]
    copies = []
    for i, part in enumerate(parts):
        at = lax.rem(y + 4 - i % 4, 4) * 2 + (core if i < 4 else 1 - core)
        copies.append(pltpu.make_async_copy(part, all_ref.at[at], sems.at[i]))
    for copy in copies:
        copy.start()
    for copy in copies:
        copy.wait()
    return 2 * y + core


def product(pos_ref, gram_refs, all_ref, at, own):
    z, x = pos_ref[5], pos_ref[6]
    sums = []
    spare = []
    for half in range(2):
        total = jnp.zeros((own.shape[0], CHUNK // 2), F32)
        extra = jnp.zeros((8, CHUNK // 2), F32)
        for a in range(4):
            for b in range(4):
                k, j = (a, b) if half == 0 else (b, a)
                j = lax.rem(x + 4 - j, 4)
                chunk = 2 * lax.rem(z + 4 - k, 4) + lax.div(j, 2)
                lanes = pl.ds(pl.multiple_of(lax.rem(j, 2) * ROWS, ROWS), ROWS)
                ref = gram_refs[4 * half + a]
                total += dot(all_ref[chunk, : own.shape[0], lanes], ref[b, :ROWS])
                extra += ref[b, ROWS:].astype(F32)[:8]
        sums.append(total)
        spare.append(extra)
    total = jnp.concatenate(sums, axis=1)
    spare = jnp.concatenate(spare, axis=1)
    return total + spare[0:1] * (own - all_ref[at, : own.shape[0]].astype(F32)) + spare[1:2] * own


def own_sum(a, b):
    ones = jnp.ones((8, CHUNK), F32)
    return lax.dot_general(
        ones, a * b, (((1,), (1,)), ((), ())), precision=lax.Precision.HIGHEST, preferred_element_type=F32
    )


def put(out_ref, block, first, second):
    out_ref[:COLS] = block.astype(BF16)
    index = lax.broadcasted_iota(jnp.int32, (16, COLS), 0)
    rows = jnp.zeros((16, COLS), F32)
    for i, own in enumerate((first, second)):
        left = own[0:1]
        for j in range(3):
            top = left.astype(BF16).astype(F32)
            rows = jnp.where(index == 3 * i + j, top, rows)
            left = left - top
    out_ref[COLS:] = jnp.concatenate([rows, jnp.zeros((16, CHUNK - COLS), F32)], axis=1).astype(BF16)


def take(all_ref):
    rows = jnp.sum(all_ref[:, COLS:].astype(F32), axis=0)
    out = []
    for i in range(2):
        row = rows[3 * i : 3 * i + 1] + (rows[3 * i + 1 : 3 * i + 2] + rows[3 * i + 2 : 3 * i + 3])
        out.append(jnp.broadcast_to(row[:, :256], (128, 256)).T[:COLS, :1])
    return out


def wide(column):
    return jnp.broadcast_to(column, (column.shape[0], 128))


def first_kernel(times, sums, own_refs, outs):
    r0 = own_refs[0][...]
    w_ref, send_ref = outs
    w0 = times(r0)
    w_ref[...] = w0
    put(send_ref, w0, own_sum(r0, r0), own_sum(r0, w0))


def second_kernel(times, sums, own_refs, outs):
    r0, w0 = (ref[...] for ref in own_refs)
    z_ref, r1_ref, w1_ref, send_ref = outs
    norm0, curve0 = sums()
    step0 = norm0 / curve0
    z0 = times(w0)
    r1 = r0 - step0 * w0
    w1 = w0 - step0 * z0
    z_ref[:, :CHUNK] = z0
    z_ref[:, CHUNK : CHUNK + 128] = wide(norm0)
    z_ref[:, CHUNK + 128 :] = wide(step0)
    r1_ref[...] = r1
    w1_ref[...] = w1
    put(send_ref, w1, own_sum(r1, r1), own_sum(r1, w1))


def third_kernel(times, sums, own_refs, outs):
    r0, w0, z0, r1, w1 = (ref[...] for ref in own_refs)
    last_ref, sums_ref = outs
    norm0, step0 = z0[:, CHUNK : CHUNK + 1], z0[:, CHUNK + 128 : CHUNK + 129]
    z0 = z0[:, :CHUNK]
    norm1, curve1 = sums()
    beta1 = norm1 / norm0
    step1 = norm1 / (curve1 - beta1 * norm1 / step0)
    p1 = r1 + beta1 * r0
    r2 = r1 - step1 * (w1 + beta1 * w0)
    last_ref[:, :CHUNK] = step0 * r0 + step1 * p1
    last_ref[:, CHUNK : 2 * CHUNK] = r2
    last_ref[:, 2 * CHUNK : 3 * CHUNK] = p1
    last_ref[:, 3 * CHUNK : 3 * CHUNK + 128] = wide(norm1)
    last_ref[:, 3 * CHUNK + 128 :] = wide(step1)
    norm2 = own_sum(r2, r2)
    w2 = w1 - step1 * (times(w1) + beta1 * z0)
    sums_ref[:, 0, :] = jnp.concatenate([norm2, own_sum(r2, w2)], axis=1)


def run(body, outs, grams, parts, pos, *owns):
    rows = parts[0].shape[0]

    def kernel(pos_ref, *refs):
        groups = []
        for n in (len(owns), len(grams), len(parts), len(outs)):
            groups.append(refs[:n])
            refs = refs[n:]
        own_refs, gram_refs, part_refs, out_refs = groups
        all_ref, sems = refs
        at = fetch(pos_ref, part_refs, all_ref, sems)
        times = lambda own: product(pos_ref, gram_refs, all_ref, at, own)
        body(times, lambda: take(all_ref), own_refs, out_refs)

    return pl.pallas_call(
        kernel,
        in_specs=[SMEM] + [VMEM] * (len(owns) + len(grams)) + [HBM] * len(parts),
        out_specs=[VMEM] * len(outs),
        out_shape=outs,
        scratch_shapes=[pltpu.VMEM((8, rows, CHUNK), BF16), pltpu.SemaphoreType.DMA((8,))],
        compiler_params=LIMIT,
        cost_estimate=cost(2 * COLS * CHUNK * 4096, 4096 * CHUNK * 2),
    )(pos, *owns, *grams, *parts)


def to_output(block):
    index = lambda y, core, z, x: ((y * 2 + core) * 4 + z) * 4 + x
    places = [(y, c, z, x) for y in range(4) for c in range(2) for z in range(4) for x in range(4)]
    odd = lax.axis_index("x") % 2
    halves = [block[:, :ROWS], block[:, ROWS:]]
    came = []
    for a in range(2):
        pairs = [
            (index(y, c, z, x), index(z, x // 2, y, 2 * c + ((x % 2) ^ a))) for y, c, z, x in places
        ]
        sent = jnp.where(odd == a, halves[0], halves[1])
        came.append(lax.ppermute(sent, ALL, pairs))
    first = jnp.where(odd == 0, came[0], came[1])
    second = jnp.where(odd == 0, came[1], came[0])
    return jnp.concatenate([first, second], axis=0).T


def shards(member_grams, member_weights):
    place = lax.axis_index(SHARD)
    chunk = lax.axis_index(MEMBER)
    pos = [lax.axis_index("y"), lax.axis_index("core"), 0, place, chunk, lax.axis_index("z"), lax.axis_index("x"), 0]
    pos = jnp.stack([jnp.asarray(p, jnp.int32) for p in pos])

    pieces = transposed(member_weights[0])
    early = gather_weights(pieces[0], True)
    ready, pieces = lax.optimization_barrier((pos, pieces))
    spread = spread_grams(ready, member_grams[0])
    grams = exchange(spread, MEMBER)
    late, grams = lax.optimization_barrier((pieces[1], grams))
    late = gather_weights(late, False)
    gram_sum = gather_plane([gather_line(half, axis) for half, axis in zip(sum_grams(pos, grams), ("x", "z"))])
    parts = []
    for piece, blocks in zip(PIECES, (early, late)):
        part = right_side_part(pos, grams, blocks)
        part = exchange(part.reshape(16, piece, CHUNK), SHARD)
        parts.append(jnp.sum(part.astype(F32), axis=0))
    r0 = jnp.concatenate(parts, axis=0)

    array = jax.ShapeDtypeStruct((COLS, CHUNK), F32)
    more = jax.ShapeDtypeStruct((COLS, CHUNK + 256), F32)
    sent = jax.ShapeDtypeStruct((COLS + 16, CHUNK), BF16)
    packed = jax.ShapeDtypeStruct((COLS, 3 * CHUNK + 256), F32)
    sums = jax.ShapeDtypeStruct((8, 1, 2 * COLS), F32)
    w0, low = run(first_kernel, (array, sent), gram_sum, gather(r0.astype(BF16)), pos, r0)
    outs = (more, array, array, sent)
    z0, r1, w1, low = run(second_kernel, outs, gram_sum, gather(low), pos, r0, w0)
    outs = (packed, sums)
    last, both = run(third_kernel, outs, gram_sum, gather(low), pos, r0, w0, z0, r1, w1)
    x1, r2, p1 = (last[:, i * CHUNK : (i + 1) * CHUNK] for i in range(3))
    norm1, step1 = last[:, 3 * CHUNK : 3 * CHUNK + 1], last[:, 3 * CHUNK + 128 : 3 * CHUNK + 129]
    both = sum(gather(both))[0, 0]
    norm2, curve2 = both[:COLS, None], both[COLS:, None]
    beta2 = norm2 / norm1
    step2 = norm2 / (curve2 - beta2 * norm2 / step1)
    p2 = r2 + beta2 * p1
    return to_output(x1 + step2 * p2)


def solution(mesh):
    fine = Mesh(mesh.devices.reshape(SIZES), ALL)

    return jax.shard_map(
        shards,
        mesh=fine,
        in_specs=(P(MEMBER, SHARD, None), P(MEMBER, SHARD, None)),
        out_specs=P(SHARD, MEMBER),
        check_vma=False,
    )
```
